128 devices in a mesh: section: 4 (over x_lo, core), tensor: 32 (over z, x_hi, y).
Axes of the slice: x: 4 (x_hi: 2, x_lo: 2; x = x_hi * 2 + x_lo), y: 4, z: 4, core: 2. Of those that a mesh axis runs over, the one named last changes fastest.
Arguments:
- tokens: bfloat16 [2, 64, 4096], replicated, may hold values from -6 to 6
- norm_gain: bfloat16 [4, 4096], replicated, may hold values from 0.25 to 1.75
- w_in: bfloat16 [4, 2, 14336, 4096], P('section', None, 'tensor'), may hold values from -0.09375 to 0.09375
- w_out: bfloat16 [4, 14336, 4096], P('section', 'tensor'), may hold values from -0.046875 to 0.046875
- backup_in: bfloat16 [4, 2, 14336, 4096], P('section', None, 'tensor'), may hold values from -0.09375 to 0.09375
- backup_out: bfloat16 [4, 14336, 4096], P('section', None, 'tensor'), may hold values from -0.046875 to 0.046875
- layer_group: int32 [4], replicated, may hold values from 0 to 3, as said below
- token_counts: int32 [2], replicated, may hold values from 1 to 64, as said below
Outputs:
- handed: bfloat16 [4, 2, 64, 4096], P('section', None, 'tensor')
The draws below stay inside these ranges and needn't reach their ends.
Inputs may be any that keep to these rules, and one draw needn't show every extreme that they name: layer_group[l] is l or l + 1. The layers that move up form one run of consecutive layers, at least one, that starts at the layer of the one group left without any layer; that group is never the last one. `token_counts`: rows of a micro-batch from its count on are padding. One micro-batch is full, with 64 real tokens; the other has at most 32.
All inputs are finite; a program needn't handle non-finite values.
Results may differ from the reference program's by a relative error of at most 0.025.
Values may be sent and summed in bfloat16 or wider, within the bound.
No kernel may reach another device: no remote copies, remote signals or barrier semaphores. Data moves between devices by JAX's collectives and lax.ppermute only.
A program may use at most 128 MiB of HBM per device.

```python
import jax
import jax.numpy as jnp
from jax import lax

D = 4096
FF = 14336
TOK = 64
MB = 2
LAYERS = 4
BLOCKS = 32


def draw_layer_group(key, part):
    key_lost, key_span = jax.random.split(jax.random.fold_in(key, 7))
    lost_group = jax.random.randint(key_lost, (), 0, LAYERS - 1)
    span_count = 1 + jax.random.randint(key_span, (), 0, LAYERS - 1 - lost_group)
    levels = jnp.arange(LAYERS, dtype=jnp.int32)
    moved_up = (levels >= lost_group) & (levels < lost_group + span_count)
    return levels + moved_up.astype(jnp.int32)


def draw_token_counts(key, part):
    key_low, key_flip = jax.random.split(jax.random.fold_in(key, 11))
    high_count = jnp.int32(TOK)
    low_count = jax.random.randint(key_low, (), 1, TOK // 2 + 1)
    flipped = jax.random.randint(key_flip, (), 0, 2)
    first = jnp.where(flipped == 1, low_count, high_count)
    second = jnp.where(flipped == 1, high_count, low_count)
    return jnp.stack([first, second]).astype(jnp.int32)


def block_levels(key, shape, cuts, smallest, high):
    gain, own = 1.0, jax.random.fold_in(key, 6)
    for dim, parts in cuts:
        steps = jnp.exp(jax.random.uniform(jax.random.fold_in(own, dim), (parts,), jnp.float32, smallest / len(cuts), high / len(cuts)))
        gain = gain * jnp.repeat(steps, shape[dim] // parts).reshape([-1 if axis == dim else 1 for axis in range(len(shape))])
    return gain


def gaussian(stream_key, extent, scale, reach, cuts=(), kind=jnp.bfloat16):
    result = jax.random.normal(stream_key, extent, jnp.float32) * scale
    if len(cuts) > 0:
        result = block_levels(stream_key, extent, cuts, -0.22, 0.18) * result
    return jnp.clip(result, min=-reach, max=reach).astype(kind)


def setup_inputs(seed: int = 0) -> dict:
    splits = jax.random.split(jax.random.key(seed), 9)
    tokens = gaussian(splits[0], (MB, TOK, D), 1.0, 6.0)
    norm_gain = jnp.clip(1.0 + 0.15 * jax.random.normal(splits[1], (LAYERS, D), jnp.float32), 0.25, 1.75).astype(jnp.bfloat16)
    w_in = gaussian(splits[2], (LAYERS, 2, FF, D), D ** -0.5, 0.09375, ((0, 4), (2, 32)))
    w_out = gaussian(splits[3], (LAYERS, FF, D), FF ** -0.5, 0.046875, ((0, 4), (1, 32)))
    backup_in = gaussian(splits[4], (LAYERS, 2, FF, D), D ** -0.5, 0.09375, ((0, 4), (2, 32)))
    backup_out = gaussian(splits[5], (LAYERS, FF, D), FF ** -0.5, 0.046875, ((0, 4), (2, 32)))
    layer_group = draw_layer_group(jax.random.fold_in(splits[8], 71), 0)
    token_counts = draw_token_counts(jax.random.fold_in(splits[8], 71), 0)
    return {"tokens": tokens, "norm_gain": norm_gain, "w_in": w_in, "w_out": w_out, "backup_in": backup_in, "backup_out": backup_out, "layer_group": layer_group, "token_counts": token_counts}


NORM_EPS = 0.25

def apply_layer(current, gain_row, w_pair, w_down, row_keep):
    wide_x = current.astype(jnp.float32)
    mean_square = lax.optimization_barrier(jnp.mean(wide_x * wide_x, axis=1, keepdims=True))
    normed = (wide_x * lax.rsqrt(mean_square + NORM_EPS) * gain_row.astype(jnp.float32)).astype(jnp.bfloat16)
    gate_part = lax.dot_general(normed, w_pair[0], (((1,), (1,)), ((), ())), preferred_element_type=jnp.float32)
    up_part = lax.dot_general(normed, w_pair[1], (((1,), (1,)), ((), ())), preferred_element_type=jnp.float32)
    hidden = (jax.nn.silu(gate_part) * up_part).astype(jnp.bfloat16)
    row_count = hidden.shape[0]
    block_width = FF // BLOCKS
    hidden_blocks = hidden.reshape(row_count, BLOCKS, block_width).astype(jnp.float32)
    down_blocks = w_down.reshape(BLOCKS, block_width, D).astype(jnp.float32)
    partial_value = jnp.einsum('rbf,bfd->brd', hidden_blocks, down_blocks)
    rounded = lax.optimization_barrier(partial_value.astype(jnp.bfloat16))
    summed = lax.optimization_barrier(jnp.sum(rounded.astype(jnp.float32), axis=0))
    return (wide_x + row_keep * summed).astype(jnp.bfloat16)

def reference(tokens, norm_gain, w_in, w_out, backup_in, backup_out, layer_group, token_counts):
    positions = jnp.arange(TOK, dtype=jnp.int32)
    row_keep = (positions[None, :] < token_counts[:, None]).astype(jnp.float32).reshape(MB * TOK, 1)
    current = tokens.reshape(MB * TOK, D)
    history = [current]
    for level in range(LAYERS):
        moved = layer_group[level] == level + 1
        spare = (level + 1) % LAYERS
        pair = jnp.where(moved, backup_in[spare], w_in[level])
        down = jnp.where(moved, backup_out[spare], w_out[level])
        current = apply_layer(current, norm_gain[level][None, :], pair, down, row_keep)
        history.append(current)
    stacked = jnp.stack(history).reshape(LAYERS + 1, MB, TOK, D)
    groups = jnp.arange(LAYERS, dtype=jnp.int32)
    reached = lax.optimization_barrier(jnp.sum((layer_group[None, :] <= groups[:, None]).astype(jnp.int32), axis=1))
    return jnp.take(stacked, reached, axis=0)
```

```python
import jax
import jax.numpy as jnp
from jax import lax
from jax.sharding import Mesh
from jax.sharding import PartitionSpec as P

TENSOR = ("tensor_0", "tensor_1", "tensor_2")
NORM_EPS = 0.25
NT = (((1,), (1,)), ((), ()))


def exchanged(value):
    return lax.all_to_all(value, TENSOR, split_axis=0, concat_axis=0, tiled=True)


def sent_to_all(value):
    return exchanged(jnp.broadcast_to(value, (lax.axis_size(TENSOR), *value.shape)))


def passed_along(block, distance):
    devices = range(lax.axis_size("section"))
    route = [(i - distance, i) for i in devices if i - distance in devices]
    return lax.ppermute(block, "section", route)


def hidden_of(columns, gain_row, w_pair):
    blocks, rows, width = columns.shape
    wide = columns.transpose(1, 0, 2).reshape(rows, blocks * width).astype(jnp.float32)
    mean_square = jnp.mean(wide * wide, axis=1, keepdims=True)
    normed = (wide * lax.rsqrt(mean_square + NORM_EPS) * gain_row.astype(jnp.float32)).astype(jnp.bfloat16)
    gate = lax.dot_general(normed, w_pair[0], NT, preferred_element_type=jnp.float32)
    up = lax.dot_general(normed, w_pair[1], NT, preferred_element_type=jnp.float32)
    return (jax.nn.silu(gate) * up).astype(jnp.bfloat16)


def shards(tokens, norm_gain, w_in, w_out, backup_in, backup_out, layer_group, token_counts):
    group = lax.axis_index("section")
    place = lax.axis_index(TENSOR)
    parts = lax.axis_size(TENSOR)
    batches, tok_rows, features = tokens.shape
    layers = layer_group.shape[0]
    half = tok_rows // 2
    rows = tok_rows + half
    width = features // parts
    share = tok_rows // parts

    first_full = token_counts[0] > half
    full = jnp.where(first_full, tokens[0], tokens[1])
    short = jnp.where(first_full, tokens[1], tokens[0])
    short_count = jnp.where(first_full, token_counts[1], token_counts[0])
    positions = jnp.arange(rows, dtype=jnp.int32)
    keep = (positions < tok_rows + short_count).astype(jnp.float32)[:, None]

    start = jnp.concatenate([full, short[:half]], axis=0)
    columns = start.reshape(rows, parts, width).transpose(1, 0, 2)

    reached = jnp.sum((layer_group <= group).astype(jnp.int32))

    def full_rows(value):
        picked = lax.dynamic_slice_in_dim(value, place * share, share, 1)
        return picked.transpose(1, 0, 2).reshape(share, features)

    def short_rows(value):
        spot = jnp.minimum(tok_rows + place * share, rows - share)
        picked = lax.dynamic_slice_in_dim(value, spot, share, 1)
        return picked.transpose(1, 0, 2).reshape(share, features)

    in_short = place * share < half
    out_full = lax.dynamic_slice_in_dim(full, place * share, share, 0)
    pad_short = lax.dynamic_slice_in_dim(short, place * share, share, 0)
    out_short = pad_short

    def own_layer(columns, own_column, gain_row):
        hidden = hidden_of(columns, gain_row, w_in[0])
        partial = jnp.dot(hidden, w_out[0], preferred_element_type=jnp.float32).astype(jnp.bfloat16)
        pieces = exchanged(partial.reshape(rows, parts, width).transpose(1, 0, 2))
        return jnp.sum(pieces.astype(jnp.float32), axis=0)

    def moved_layer(columns, own_column, gain_row):
        hidden = hidden_of(columns, gain_row, backup_in[0])
        everyone = sent_to_all(hidden)
        full_hidden = everyone.transpose(1, 0, 2).reshape(rows, -1)
        return jnp.dot(full_hidden, backup_out[0], preferred_element_type=jnp.float32)

    for level in range(layers - 1):
        own_column = lax.dynamic_index_in_dim(columns, place, 0, keepdims=False)
        gain_row = norm_gain[level][None, :]
        moved = layer_group[level] == level + 1
        summed = lax.cond(moved, moved_layer, own_layer, columns, own_column, gain_row)
        fresh = (own_column.astype(jnp.float32) + keep * summed).astype(jnp.bfloat16)
        active = layer_group[level]
        near = passed_along(fresh, 1)
        far = passed_along(fresh, 2)
        fresh = jnp.where(group == active, fresh, jnp.where(group == active + 1, near, far))
        columns = sent_to_all(fresh)
        here = reached == level + 1
        out_full = jnp.where(here, full_rows(columns), out_full)
        out_short = jnp.where(here & in_short, short_rows(columns), out_short)

    hidden = hidden_of(columns, norm_gain[layers - 1][None, :], w_in[0])
    partial = jnp.dot(hidden, w_out[0], preferred_element_type=jnp.float32).astype(jnp.bfloat16)
    full_part = partial[:tok_rows].reshape(parts, share, features)
    short_part = jnp.pad(partial[tok_rows:].reshape(parts // 2, share, features), ((0, parts // 2), (0, 0), (0, 0)))
    pieces = exchanged(jnp.concatenate([full_part, short_part], axis=1))
    summed = jnp.sum(pieces.astype(jnp.float32), axis=0)
    here = reached == layers
    last_full = (full_rows(columns).astype(jnp.float32) + summed[:share]).astype(jnp.bfloat16)
    spots = place * share + jnp.arange(share, dtype=jnp.int32)
    keep_short = (spots < short_count).astype(jnp.float32)[:, None]
    last_short = (short_rows(columns).astype(jnp.float32) + keep_short * summed[share:]).astype(jnp.bfloat16)
    out_full = jnp.where(here, last_full, out_full)
    out_short = jnp.where(here & in_short, last_short, out_short)
    handed = jnp.where(first_full, jnp.stack([out_full, out_short]), jnp.stack([out_short, out_full]))
    return handed[None]


def solution(mesh):
    finer = Mesh(
        mesh.devices.reshape(mesh.shape["section"], 4, 2, 4),
        ("section", "tensor_0", "tensor_1", "tensor_2"),
    )
    return jax.shard_map(
        shards,
        mesh=finer,
        in_specs=(
            P(),
            P(),
            P("section", None, TENSOR, None),
            P("section", TENSOR, None),
            P("section", None, TENSOR, None),
            P("section", None, TENSOR),
            P(),
            P(),
        ),
        out_specs=P("section", None, TENSOR, None),
        check_vma=False,
    )
```

```python
import jax
import jax.numpy as jnp
from jax import lax
from jax.sharding import Mesh
from jax.sharding import PartitionSpec as P

TENSOR = ("tensor_0", "tensor_1", "tensor_2")
NORM_EPS = 0.25
NT = (((1,), (1,)), ((), ()))


def exchanged(value):
    return lax.all_to_all(value, TENSOR, split_axis=0, concat_axis=0, tiled=True)


def sent_to_all(value):
    return exchanged(jnp.broadcast_to(value, (lax.axis_size(TENSOR), *value.shape)))


def passed_along(block, distance):
    devices = range(lax.axis_size("section"))
    route = [(i - distance, i) for i in devices if i - distance in devices]
    return lax.ppermute(block, "section", route)


def hidden_of(columns, gain_row, w_pair):
    blocks, rows, width = columns.shape
    wide = columns.transpose(1, 0, 2).reshape(rows, blocks * width).astype(jnp.float32)
    mean_square = jnp.mean(wide * wide, axis=1, keepdims=True)
    normed = (wide * lax.rsqrt(mean_square + NORM_EPS) * gain_row.astype(jnp.float32)).astype(jnp.bfloat16)
    gate = lax.dot_general(normed, w_pair[0], NT, preferred_element_type=jnp.float32)
    up = lax.dot_general(normed, w_pair[1], NT, preferred_element_type=jnp.float32)
    return (jax.nn.silu(gate) * up).astype(jnp.bfloat16)


def shards(tokens, norm_gain, w_in, w_out, backup_in, backup_out, layer_group, token_counts):
    group = lax.axis_index("section")
    place = lax.axis_index(TENSOR)
    parts = lax.axis_size(TENSOR)
    batches, tok_rows, features = tokens.shape
    layers = layer_group.shape[0]
    levels = jnp.arange(layers, dtype=jnp.int32)
    half = tok_rows // 2
    rows = tok_rows + half
    width = features // parts
    share = tok_rows // parts

    first_full = token_counts[0] > half
    full = jnp.where(first_full, tokens[0], tokens[1])
    short = jnp.where(first_full, tokens[1], tokens[0])
    short_count = jnp.where(first_full, token_counts[1], token_counts[0])
    positions = jnp.arange(rows, dtype=jnp.int32)
    keep = (positions < tok_rows + short_count).astype(jnp.float32)[:, None]

    start = jnp.concatenate([full, short[:half]], axis=0)
    columns = start.reshape(rows, parts, width).transpose(1, 0, 2)

    reached = jnp.sum((layer_group <= group).astype(jnp.int32))
    runs_moved = jnp.sum(((levels == group - 1) & (layer_group == group)).astype(jnp.int32)) > 0
    gain_rows = [norm_gain[level][None, :] for level in range(layers)]

    moved_down = lax.cond(
        runs_moved,
        lambda held: exchanged(held.reshape(parts, -1, width)),
        lambda held: jnp.zeros((parts, held.shape[0] // parts, width), held.dtype),
        backup_out[0],
    )

    def scattered(pieces):
        return jnp.sum(exchanged(pieces).astype(jnp.float32), axis=0)

    def idle_layer(columns, gain_row, moved_down):
        return jnp.zeros((rows, width), jnp.bfloat16)

    def finished(columns, summed):
        own_column = lax.dynamic_index_in_dim(columns, place, 0, keepdims=False)
        return (own_column.astype(jnp.float32) + keep * summed).astype(jnp.bfloat16)

    def own_layer(columns, gain_row, moved_down):
        hidden = hidden_of(columns, gain_row, w_in[0])
        partial = jnp.dot(hidden, w_out[0], preferred_element_type=jnp.float32).astype(jnp.bfloat16)
        return finished(columns, scattered(partial.reshape(rows, parts, width).transpose(1, 0, 2)))

    def moved_layer(columns, gain_row, moved_down):
        hidden = hidden_of(columns, gain_row, backup_in[0])
        pieces = jnp.einsum("rf,bfd->brd", hidden, moved_down, preferred_element_type=jnp.float32)
        return finished(columns, scattered(pieces.astype(jnp.bfloat16)))

    def hand_rows(columns, kept):
        full_part = kept[:tok_rows].reshape(parts, share, width)
        short_part = jnp.pad(kept[tok_rows:].reshape(parts // 2, share, width), ((0, parts // 2), (0, 0), (0, 0)))
        pieces = exchanged(jnp.concatenate([full_part, short_part], axis=1))
        return pieces.transpose(1, 0, 2).reshape(2 * share, features)

    def stay(fresh, hop_from):
        return fresh

    def step_one(fresh, hop_from):
        near = passed_along(fresh, 1)
        return jnp.where(group == hop_from, fresh, near)

    def step_two(fresh, hop_from):
        far = passed_along(fresh, 2)
        near = passed_along(fresh, 1)
        return jnp.where(group == hop_from, fresh, jnp.where(group == hop_from + 1, near, far))

    spots = place * share + jnp.arange(share, dtype=jnp.int32)
    first_rows = jnp.concatenate(
        [
            lax.dynamic_slice_in_dim(full, place * share, share, 0),
            lax.dynamic_slice_in_dim(short, place * share, share, 0),
        ]
    )
    kept = lax.dynamic_index_in_dim(columns, place, 0, keepdims=False)
    for level in range(layers - 1):
        hop_from = layer_group[level]
        hop_to = layer_group[level + 1]
        runs = jnp.where(group == hop_from, jnp.where(hop_from == level, 1, 2), 0)
        fresh = lax.switch(runs, [idle_layer, own_layer, moved_layer], columns, gain_rows[level], moved_down)
        fresh = lax.switch(hop_to - hop_from, [stay, step_one, step_two], fresh, hop_from)
        kept = jnp.where(reached == level + 1, fresh, kept)
        columns = lax.cond(group == hop_to, lambda fresh, columns: sent_to_all(fresh), lambda fresh, columns: columns, fresh, columns)

    def last_layer(columns, kept):
        hidden = hidden_of(columns, gain_rows[layers - 1], w_in[0])
        partial = jnp.dot(hidden, w_out[0], preferred_element_type=jnp.float32).astype(jnp.bfloat16)
        full_part = partial[:tok_rows].reshape(parts, share, features)
        short_part = jnp.pad(partial[tok_rows:].reshape(parts // 2, share, features), ((0, parts // 2), (0, 0), (0, 0)))
        pieces = exchanged(jnp.concatenate([full_part, short_part], axis=1))
        summed = jnp.sum(pieces.astype(jnp.float32), axis=0)
        held_full = lax.dynamic_slice_in_dim(columns, place * share, share, 1)
        spot = jnp.minimum(tok_rows + place * share, rows - share)
        held_short = lax.dynamic_slice_in_dim(columns, spot, share, 1)
        held = jnp.concatenate([held_full, held_short], axis=1).transpose(1, 0, 2).reshape(2 * share, features)
        keep_rows = jnp.concatenate([jnp.ones((share,), jnp.bool_), spots < short_count]).astype(jnp.float32)[:, None]
        return (held.astype(jnp.float32) + keep_rows * summed).astype(jnp.bfloat16)

    out_rows = lax.cond(group == layer_group[layers - 1], last_layer, hand_rows, columns, kept)
    padding = (place * share >= half) & (jnp.arange(2 * share, dtype=jnp.int32) >= share)
    out_rows = jnp.where(padding[:, None], first_rows, out_rows)
    out_full, out_short = out_rows[:share], out_rows[share:]
    handed = jnp.where(first_full, jnp.stack([out_full, out_short]), jnp.stack([out_short, out_full]))
    return handed[None]


def solution(mesh):
    finer = Mesh(
        mesh.devices.reshape(mesh.shape["section"], 4, 2, 4),
        ("section", "tensor_0", "tensor_1", "tensor_2"),
    )
    return jax.shard_map(
        shards,
        mesh=finer,
        in_specs=(
            P(),
            P(),
            P("section", None, TENSOR, None),
            P("section", TENSOR, None),
            P("section", None, TENSOR, None),
            P("section", None, TENSOR),
            P(),
            P(),
        ),
        out_specs=P("section", None, TENSOR, None),
        check_vma=False,
    )
```

```python
import jax
import jax.numpy as jnp
from jax import lax
from jax.experimental import pallas as pl
from jax.experimental.pallas import tpu as pltpu
from jax.sharding import Mesh
from jax.sharding import PartitionSpec as P

TENSOR = ("tensor_0", "tensor_1", "tensor_2")
NORM_EPS = 0.25
NT = (((1,), (1,)), ((), ()))
NN = (((1,), (0,)), ((), ()))
DOWN_CUTS = 4


def exchanged(value):
    return lax.all_to_all(value, TENSOR, split_axis=0, concat_axis=0, tiled=True)


def sent_to_all(value):
    return exchanged(jnp.broadcast_to(value, (lax.axis_size(TENSOR), *value.shape)))


def passed_along(block, distance):
    devices = range(lax.axis_size("section"))
    route = [(i - distance, i) for i in devices if i - distance in devices]
    return lax.ppermute(block, "section", route)


def unwritten(shape, dtype):
    return pl.pallas_call(
        lambda out: None,
        out_shape=jax.ShapeDtypeStruct(shape, dtype),
        out_specs=pl.BlockSpec(memory_space=pl.ANY),
    )()


def layer_kernel(moved, x, gain, own_in, kept_in, own_out, kept_out, out, pair, down, normed, hidden, in_sems, out_sems):
    blocks, rows, width = x.shape
    units, features = down.shape
    cuts = ((0, 256), (256, units - 256))
    span = features // DOWN_CUTS
    per_cut = span // width
    moves = moved[0] == 1

    def start_in(source):
        for cut, (at, size) in enumerate(cuts):
            for half in range(2):
                pltpu.make_async_copy(
                    source.at[0, half, pl.ds(at, size), :], pair.at[half, pl.ds(at, size), :], in_sems.at[cut, half]
                ).start()

    @pl.when(moves)
    def _():
        start_in(kept_in)
        for cut in range(DOWN_CUTS):
            for block in range(cut * per_cut, (cut + 1) * per_cut):
                pltpu.make_async_copy(
                    kept_out.at[block], down.at[:, pl.ds(block * width, width)], out_sems.at[cut]
                ).start()

    @pl.when(jnp.logical_not(moves))
    def _():
        start_in(own_in)
        for cut in range(DOWN_CUTS):
            place = pl.ds(cut * span, span)
            pltpu.make_async_copy(own_out.at[0, :, place], down.at[:, place], out_sems.at[cut]).start()

    def add_square(block, total):
        wide = x[block].astype(jnp.float32)
        return total + wide * wide

    total = lax.fori_loop(0, blocks, add_square, jnp.zeros((rows, width), jnp.float32))
    scale = lax.rsqrt(jnp.sum(total, axis=1, keepdims=True) * (1.0 / features) + NORM_EPS)

    def scale_block(block, carry):
        value = x[block].astype(jnp.float32) * scale * gain[pl.ds(block, 1), :]
        normed[:, pl.ds(pl.multiple_of(block * width, width), width)] = value.astype(jnp.bfloat16)
        return carry

    lax.fori_loop(0, blocks, scale_block, 0)
    for cut, (at, size) in enumerate(cuts):
        here = pl.ds(at, size)
        parts = []
        for half in range(2):
            arrived = pair.at[half, here, :]
            pltpu.make_async_copy(arrived, arrived, in_sems.at[cut, half]).wait()
            parts.append(lax.dot_general(normed[...], pair[half, here, :], NT, preferred_element_type=jnp.float32))
        gate, up = parts
        hidden[:, here] = (gate / (1.0 + jnp.exp(-gate)) * up).astype(jnp.bfloat16)
    for cut in range(DOWN_CUTS):
        place = pl.ds(cut * span, span)
        arrived = down.at[:, place]
        pltpu.make_async_copy(arrived, arrived, out_sems.at[cut]).wait()
        result = lax.dot_general(hidden[...], down[:, place], NN, preferred_element_type=jnp.float32)
        for block in range(per_cut):
            out[cut * per_cut + block] = result[:, block * width : (block + 1) * width].astype(jnp.bfloat16)


def partial_sums(moved, columns, gain, own_in, kept_in, own_out, kept_out):
    blocks, rows, width = columns.shape
    units = own_out.shape[1]
    features = blocks * width
    vmem = pl.BlockSpec(memory_space=pltpu.VMEM)
    anywhere = pl.BlockSpec(memory_space=pl.ANY)
    return pl.pallas_call(
        layer_kernel,
        out_shape=jax.ShapeDtypeStruct(columns.shape, jnp.bfloat16),
        in_specs=[pl.BlockSpec(memory_space=pltpu.SMEM), vmem, vmem, anywhere, anywhere, anywhere, anywhere],
        out_specs=vmem,
        scratch_shapes=[
            pltpu.VMEM((2, units, features), jnp.bfloat16),
            pltpu.VMEM((units, features), jnp.bfloat16),
            pltpu.VMEM((rows, features), jnp.bfloat16),
            pltpu.VMEM((rows, units), jnp.bfloat16),
            pltpu.SemaphoreType.DMA((2, 2)),
            pltpu.SemaphoreType.DMA((DOWN_CUTS,)),
        ],
        compiler_params=pltpu.CompilerParams(vmem_limit_bytes=32 * 1024 * 1024),
    )(moved, columns, gain, own_in, kept_in, own_out, kept_out)


def shards(tokens, norm_gain, w_in, w_out, backup_in, backup_out, layer_group, token_counts):
    group = lax.axis_index("section")
    place = lax.axis_index(TENSOR)
    parts = lax.axis_size(TENSOR)
    batches, tok_rows, features = tokens.shape
    layers = layer_group.shape[0]
    levels = jnp.arange(layers, dtype=jnp.int32)
    half = tok_rows // 2
    rows = tok_rows + half
    width = features // parts
    share = tok_rows // parts

    first_full = token_counts[0] > half
    full = jnp.where(first_full, tokens[0], tokens[1])
    short = jnp.where(first_full, tokens[1], tokens[0])
    short_count = jnp.where(first_full, token_counts[1], token_counts[0])
    positions = jnp.arange(rows, dtype=jnp.int32)
    keep = (positions < tok_rows + short_count).astype(jnp.float32)[:, None]
    spots = place * share + jnp.arange(share, dtype=jnp.int32)

    start = jnp.concatenate([full, short[:half]], axis=0)
    columns = start.reshape(rows, parts, width).transpose(1, 0, 2)
    gains = norm_gain.astype(jnp.float32).reshape(layers, parts, width)

    reached = jnp.sum((layer_group <= group).astype(jnp.int32))
    runs_moved = jnp.sum(((levels == group - 1) & (layer_group == group)).astype(jnp.int32)) > 0

    moved_down = lax.cond(
        runs_moved,
        lambda held: exchanged(held.reshape(parts, -1, width)),
        lambda held: unwritten((parts, held.shape[0] // parts, width), held.dtype),
        backup_out[0],
    )

    def idle_layer(columns, gain, moved):
        return lax.dynamic_index_in_dim(columns, place, 0, keepdims=False)

    def active_layer(columns, gain, moved):
        pieces = partial_sums(moved, columns, gain, w_in, backup_in, w_out, moved_down)
        summed = jnp.sum(exchanged(pieces).astype(jnp.float32), axis=0)
        own_column = lax.dynamic_index_in_dim(columns, place, 0, keepdims=False)
        return (own_column.astype(jnp.float32) + keep * summed).astype(jnp.bfloat16)

    def stay(fresh, hop_from):
        return fresh

    def step_one(fresh, hop_from):
        near = passed_along(fresh, 1)
        return jnp.where(group == hop_from, fresh, near)

    def step_two(fresh, hop_from):
        far = passed_along(fresh, 2)
        near = passed_along(fresh, 1)
        return jnp.where(group == hop_from, fresh, jnp.where(group == hop_from + 1, near, far))

    def run_level(level, state):
        columns, kept = state
        hop_from = lax.dynamic_index_in_dim(layer_group, level, 0, keepdims=False)
        hop_to = lax.dynamic_index_in_dim(layer_group, level + 1, 0, keepdims=False)
        gain = lax.dynamic_index_in_dim(gains, level, 0, keepdims=False)
        moved = (hop_from == level + 1).astype(jnp.int32)[None]
        fresh = lax.cond(group == hop_from, active_layer, idle_layer, columns, gain, moved)
        fresh = lax.switch(hop_to - hop_from, [stay, step_one, step_two], fresh, hop_from)
        kept = jnp.where(reached == level + 1, fresh, kept)
        columns = lax.cond(group == hop_to, lambda fresh, columns: sent_to_all(fresh), lambda fresh, columns: columns, fresh, columns)
        return columns, kept

    kept = lax.dynamic_index_in_dim(columns, place, 0, keepdims=False)
    columns, kept = lax.fori_loop(0, layers - 1, run_level, (columns, kept))

    def hand_rows(columns, kept):
        full_part = kept[:tok_rows].reshape(parts, share, width)
        short_part = jnp.pad(kept[tok_rows:].reshape(parts // 2, share, width), ((0, parts // 2), (0, 0), (0, 0)))
        pieces = exchanged(jnp.concatenate([full_part, short_part], axis=1))
        return pieces.transpose(1, 0, 2).reshape(2 * share, features)

    def last_layer(columns, kept):
        pieces = partial_sums(jnp.zeros((1,), jnp.int32), columns, gains[layers - 1], w_in, backup_in, w_out, moved_down)
        partial = pieces.transpose(1, 0, 2).reshape(rows, features)
        full_part = partial[:tok_rows].reshape(parts, share, features)
        short_part = jnp.pad(partial[tok_rows:].reshape(parts // 2, share, features), ((0, parts // 2), (0, 0), (0, 0)))
        pieces = exchanged(jnp.concatenate([full_part, short_part], axis=1))
        summed = jnp.sum(pieces.astype(jnp.float32), axis=0)
        held_full = lax.dynamic_slice_in_dim(columns, place * share, share, 1)
        spot = jnp.minimum(tok_rows + place * share, rows - share)
        held_short = lax.dynamic_slice_in_dim(columns, spot, share, 1)
        held = jnp.concatenate([held_full, held_short], axis=1).transpose(1, 0, 2).reshape(2 * share, features)
        keep_rows = jnp.concatenate([jnp.ones((share,), jnp.bool_), spots < short_count]).astype(jnp.float32)[:, None]
        return (held.astype(jnp.float32) + keep_rows * summed).astype(jnp.bfloat16)

    out_rows = lax.cond(group == layer_group[layers - 1], last_layer, hand_rows, columns, kept)
    first_rows = jnp.concatenate(
        [
            lax.dynamic_slice_in_dim(full, place * share, share, 0),
            lax.dynamic_slice_in_dim(short, place * share, share, 0),
        ]
    )
    padding = (place * share >= half) & (jnp.arange(2 * share, dtype=jnp.int32) >= share)
    out_rows = jnp.where(padding[:, None], first_rows, out_rows)
    out_full, out_short = out_rows[:share], out_rows[share:]
    handed = jnp.where(first_full, jnp.stack([out_full, out_short]), jnp.stack([out_short, out_full]))
    return handed[None]


def solution(mesh):
    finer = Mesh(
        mesh.devices.reshape(mesh.shape["section"], 4, 2, 4),
        ("section", "tensor_0", "tensor_1", "tensor_2"),
    )
    return jax.shard_map(
        shards,
        mesh=finer,
        in_specs=(
            P(),
            P(),
            P("section", None, TENSOR, None),
            P("section", TENSOR, None),
            P("section", None, TENSOR, None),
            P("section", None, TENSOR),
            P(),
            P(),
        ),
        out_specs=P("section", None, TENSOR, None),
        check_vma=False,
    )
```

```python
import functools

import jax
import jax.numpy as jnp
from jax import lax
from jax.experimental import pallas as pl
from jax.experimental.pallas import tpu as pltpu
from jax.sharding import Mesh
from jax.sharding import PartitionSpec as P

TENSOR = ("tensor_0", "tensor_1", "tensor_2")
NORM_EPS = 0.25
NT = (((1,), (1,)), ((), ()))
NN = (((1,), (0,)), ((), ()))
IN_CUTS = 4
OUT_CUTS = 4
AHEAD = 2


def exchanged(value):
    return lax.all_to_all(value, TENSOR, split_axis=0, concat_axis=0, tiled=True)


def sent_to_all(value):
    return exchanged(jnp.broadcast_to(value, (lax.axis_size(TENSOR), *value.shape)))


def passed_along(block, distance):
    devices = range(lax.axis_size("section"))
    route = [(i - distance, i) for i in devices if i - distance in devices]
    return lax.ppermute(block, "section", route)


def unwritten(shape, dtype):
    return pl.pallas_call(
        lambda out: None,
        out_shape=jax.ShapeDtypeStruct(shape, dtype),
        out_specs=pl.BlockSpec(memory_space=pl.ANY),
    )()


def first_kernel(full, tokens, out, rows_in, sems):
    blocks, rows, width = out.shape
    tok_rows = tokens.shape[1]
    copies = [
        pltpu.make_async_copy(tokens.at[full[0]], rows_in.at[pl.ds(0, tok_rows)], sems.at[0]),
        pltpu.make_async_copy(
            tokens.at[1 - full[0], pl.ds(0, rows - tok_rows)], rows_in.at[pl.ds(tok_rows, rows - tok_rows)], sems.at[1]
        ),
    ]
    for copy in copies:
        copy.start()
    for copy in copies:
        copy.wait()
    for block in range(blocks):
        out[block] = rows_in[:, block * width : (block + 1) * width]


def first_columns(full, tokens, blocks, rows):
    features = tokens.shape[2]
    return pl.pallas_call(
        first_kernel,
        out_shape=pltpu.VMEM((blocks, rows, features // blocks), tokens.dtype),
        in_specs=[pl.BlockSpec(memory_space=pltpu.SMEM), pl.BlockSpec(memory_space=pl.ANY)],
        out_specs=pl.BlockSpec(memory_space=pltpu.VMEM),
        scratch_shapes=[pltpu.VMEM((rows, features), tokens.dtype), pltpu.SemaphoreType.DMA((2,))],
    )(full, tokens)


def layer_kernel(level, moved, x, gain, own_in, kept_in, own_out, kept_out, out, pair, down, normed, hidden, in_sems, out_sems):
    blocks, rows, width = x.shape
    units, features = down.shape
    in_span = features // IN_CUTS
    out_span = features // OUT_CUTS
    per_cut = out_span // width
    moves = moved[0] == 1

    def in_place(cut):
        return pl.ds(cut * in_span, in_span)

    def out_place(cut):
        return pl.ds(cut * out_span, out_span)

    def start(step):
        if step < IN_CUTS:
            here, sem = in_place(step), in_sems.at[step]

            @pl.when(moves)
            def _():
                pltpu.make_async_copy(kept_in.at[0, :, :, here], pair.at[:, :, here], sem).start()

            @pl.when(jnp.logical_not(moves))
            def _():
                pltpu.make_async_copy(own_in.at[0, :, :, here], pair.at[:, :, here], sem).start()

        elif step < IN_CUTS + OUT_CUTS:
            cut = step - IN_CUTS
            here, sem = out_place(cut), out_sems.at[cut]

            @pl.when(moves)
            def _():
                for block in range(cut * per_cut, (cut + 1) * per_cut):
                    pltpu.make_async_copy(kept_out.at[block], down.at[:, pl.ds(block * width, width)], sem).start()

            @pl.when(jnp.logical_not(moves))
            def _():
                pltpu.make_async_copy(own_out.at[0, :, here], down.at[:, here], sem).start()

    for step in range(AHEAD):
        start(step)

    def add_square(block, total):
        wide = x[block].astype(jnp.float32)
        return total + wide * wide

    total = lax.fori_loop(0, blocks, add_square, jnp.zeros((rows, width), jnp.float32), unroll=4)
    scale = lax.rsqrt(jnp.sum(total, axis=1, keepdims=True) * (1.0 / features) + NORM_EPS)

    def scale_block(block, carry):
        spot = pl.ds(pl.multiple_of(block * width, width), width)
        row = gain[:, spot].astype(jnp.float32)[level : level + 1]
        normed[:, spot] = (x[block].astype(jnp.float32) * scale * row).astype(jnp.bfloat16)
        return carry

    lax.fori_loop(0, blocks, scale_block, 0, unroll=4)
    sums = [jnp.zeros((rows, units), jnp.float32)] * 2
    for cut in range(IN_CUTS):
        here = in_place(cut)
        arrived = pair.at[:, :, here]
        pltpu.make_async_copy(arrived, arrived, in_sems.at[cut]).wait()
        start(cut + AHEAD)
        for half in range(2):
            sums[half] += lax.dot_general(normed[:, here], pair[half, :, here], NT, preferred_element_type=jnp.float32)
    gate, up = sums
    hidden[...] = (gate / (1.0 + jnp.exp(-gate)) * up).astype(jnp.bfloat16)
    for cut in range(OUT_CUTS):
        here = out_place(cut)
        arrived = down.at[:, here]
        pltpu.make_async_copy(arrived, arrived, out_sems.at[cut]).wait()
        start(IN_CUTS + cut + AHEAD)
        result = lax.dot_general(hidden[...], down[:, here], NN, preferred_element_type=jnp.float32)
        for block in range(per_cut):
            out[cut * per_cut + block] = result[:, block * width : (block + 1) * width].astype(jnp.bfloat16)


def partial_sums(level, moved, columns, gain, own_in, kept_in, own_out, kept_out):
    blocks, rows, width = columns.shape
    units = own_out.shape[1]
    features = blocks * width
    vmem = pl.BlockSpec(memory_space=pltpu.VMEM)
    anywhere = pl.BlockSpec(memory_space=pl.ANY)
    return pl.pallas_call(
        functools.partial(layer_kernel, level),
        out_shape=pltpu.VMEM(columns.shape, jnp.bfloat16),
        in_specs=[pl.BlockSpec(memory_space=pltpu.SMEM), vmem, vmem, anywhere, anywhere, anywhere, anywhere],
        out_specs=vmem,
        scratch_shapes=[
            pltpu.VMEM((2, units, features), jnp.bfloat16),
            pltpu.VMEM((units, features), jnp.bfloat16),
            pltpu.VMEM((rows, features), jnp.bfloat16),
            pltpu.VMEM((rows, units), jnp.bfloat16),
            pltpu.SemaphoreType.DMA((IN_CUTS,)),
            pltpu.SemaphoreType.DMA((OUT_CUTS,)),
        ],
        compiler_params=pltpu.CompilerParams(vmem_limit_bytes=32 * 1024 * 1024),
    )(moved, columns, gain, own_in, kept_in, own_out, kept_out)


def shards(tokens, norm_gain, w_in, w_out, backup_in, backup_out, layer_group, token_counts):
    group = lax.axis_index("section")
    place = lax.axis_index(TENSOR)
    parts = lax.axis_size(TENSOR)
    batches, tok_rows, features = tokens.shape
    layers = layer_group.shape[0]
    levels = jnp.arange(layers, dtype=jnp.int32)
    half = tok_rows // 2
    rows = tok_rows + half
    width = features // parts
    share = tok_rows // parts

    first_full = token_counts[0] > half
    full = jnp.where(first_full, 0, 1)
    short_count = jnp.where(first_full, token_counts[1], token_counts[0])
    positions = jnp.arange(rows, dtype=jnp.int32)
    keep = (positions < tok_rows + short_count).astype(jnp.float32)[:, None]
    spots = place * share + jnp.arange(share, dtype=jnp.int32)
    columns = first_columns(full[None], tokens, parts, rows)

    reached = jnp.sum((layer_group <= group).astype(jnp.int32))
    runs_moved = jnp.sum(((levels == group - 1) & (layer_group == group)).astype(jnp.int32)) > 0

    moved_down = lax.cond(
        runs_moved,
        lambda held: exchanged(held.reshape(parts, -1, width)),
        lambda held: unwritten((parts, held.shape[0] // parts, width), held.dtype),
        backup_out[0],
    )

    def finished(level, columns, moved):
        own_column = lax.dynamic_index_in_dim(columns, place, 0, keepdims=False)
        pieces = partial_sums(level, moved, columns, norm_gain, w_in, backup_in, w_out, moved_down)
        pieces, own_column = lax.optimization_barrier((pieces, own_column))
        summed = jnp.sum(exchanged(pieces).astype(jnp.float32), axis=0)
        return (own_column.astype(jnp.float32) + keep * summed).astype(jnp.bfloat16)

    def stay(fresh, hop_from):
        return fresh

    def step_one(fresh, hop_from):
        near = passed_along(fresh, 1)
        return jnp.where(group == hop_from, fresh, near)

    def step_two(fresh, hop_from):
        far = passed_along(fresh, 2)
        near = passed_along(fresh, 1)
        return jnp.where(group == hop_from, fresh, jnp.where(group == hop_from + 1, near, far))

    kept = lax.dynamic_index_in_dim(columns, place, 0, keepdims=False)
    fresh = kept
    for level in range(layers - 1):
        hop_from = layer_group[level]
        hop_to = layer_group[level + 1]
        moved = (hop_from == level + 1).astype(jnp.int32)[None]
        if level == 0:
            run = lambda fresh, moved: finished(0, columns, moved)
        else:
            run = lambda fresh, moved, level=level: finished(level, sent_to_all(fresh), moved)
        fresh = lax.cond(group == hop_from, run, lambda fresh, moved: fresh, fresh, moved)
        fresh = lax.switch(hop_to - hop_from, [stay, step_one, step_two], fresh, hop_from)
        kept = jnp.where(reached == level + 1, fresh, kept)

    def hand_rows(fresh, kept):
        full_part = kept[:tok_rows].reshape(parts, share, width)
        short_part = jnp.pad(kept[tok_rows:].reshape(parts // 2, share, width), ((0, parts // 2), (0, 0), (0, 0)))
        pieces = exchanged(jnp.concatenate([full_part, short_part], axis=1))
        return pieces.transpose(1, 0, 2).reshape(2 * share, features)

    def last_layer(fresh, kept):
        columns = sent_to_all(fresh)
        moved = jnp.zeros((1,), jnp.int32)
        pieces = partial_sums(layers - 1, moved, columns, norm_gain, w_in, backup_in, w_out, moved_down)
        partial = pieces.transpose(1, 0, 2).reshape(rows, features)
        full_part = partial[:tok_rows].reshape(parts, share, features)
        short_part = jnp.pad(partial[tok_rows:].reshape(parts // 2, share, features), ((0, parts // 2), (0, 0), (0, 0)))
        pieces = exchanged(jnp.concatenate([full_part, short_part], axis=1))
        summed = jnp.sum(pieces.astype(jnp.float32), axis=0)
        held_full = lax.dynamic_slice_in_dim(columns, place * share, share, 1)
        spot = jnp.minimum(tok_rows + place * share, rows - share)
        held_short = lax.dynamic_slice_in_dim(columns, spot, share, 1)
        held = jnp.concatenate([held_full, held_short], axis=1).transpose(1, 0, 2).reshape(2 * share, features)
        keep_rows = jnp.concatenate([jnp.ones((share,), jnp.bool_), spots < short_count]).astype(jnp.float32)[:, None]
        return (held.astype(jnp.float32) + keep_rows * summed).astype(jnp.bfloat16)

    out_rows = lax.cond(group == layer_group[layers - 1], last_layer, hand_rows, fresh, kept)
    first_rows = jnp.concatenate(
        [
            lax.dynamic_slice(tokens, (full, place * share, 0), (1, share, features))[0],
            lax.dynamic_slice(tokens, (1 - full, place * share, 0), (1, share, features))[0],
        ]
    )
    padding = (place * share >= half) & (jnp.arange(2 * share, dtype=jnp.int32) >= share)
    out_rows = jnp.where(padding[:, None], first_rows, out_rows)
    out_full, out_short = out_rows[:share], out_rows[share:]
    handed = jnp.where(first_full, jnp.stack([out_full, out_short]), jnp.stack([out_short, out_full]))
    return handed[None]


def solution(mesh):
    finer = Mesh(
        mesh.devices.reshape(mesh.shape["section"], 4, 2, 4),
        ("section", "tensor_0", "tensor_1", "tensor_2"),
    )
    return jax.shard_map(
        shards,
        mesh=finer,
        in_specs=(
            P(),
            P(),
            P("section", None, TENSOR, None),
            P("section", TENSOR, None),
            P("section", None, TENSOR, None),
            P("section", None, TENSOR),
            P(),
            P(),
        ),
        out_specs=P("section", None, TENSOR, None),
        check_vma=False,
    )
```
